32 devices in a mesh: rep: 2 (over x), tp: 4 (over y, core), sub: 4 (over z).
Axes of the slice: x: 2, y: 2, z: 4, core: 2. Of those that a mesh axis runs over, the one named last changes fastest.
Arguments:
- acts: bfloat16 [2048, 16384], P(('rep', 'tp'), 'sub'), parts along dimension 0, may hold values from -6 to 6
- q_src: bfloat16 [32768, 16384], P(('rep', 'sub'), 'tp'), parts along dimension 0, may hold values from -0.046875 to 0.046875
- kv_src: bfloat16 [32768, 2048], P(('rep', 'sub'), 'tp'), parts along dimension 0, may hold values from -0.046875 to 0.046875
- q_src_heads: int32 [128], replicated, may hold values from 0 to 127, as said below
- q_tgt_heads: int32 [128], replicated, may hold values from 0 to 127, as said below
- kv_tgt_heads: int32 [16], replicated, may hold values from 0 to 7, as said below
Outputs:
- q_new: bfloat16 [32768, 16384], P(('rep', 'sub'), 'tp'), parts along dimension 0
- kv_new: bfloat16 [32768, 4096], P(('rep', 'sub'), 'tp'), parts along dimension 0
- qkv: bfloat16 [2048, 20480], P(('rep', 'sub'), 'tp'), parts along dimension 0
The draws below stay inside these ranges and needn't reach their ends.
There are 2 independent parts, one for each index of `rep`. The reference program is written for one: setup_inputs(seed, part) draws one part's arguments, and reference() takes and returns one part's arrays. A program takes and returns all parts, laid end to end along the dimension named above; an argument that names none is the same for every part. Nothing has to cross between parts.
Inputs may be any that keep to these rules, and one draw needn't show every extreme that they name: q_src_heads and q_tgt_heads are permutations. Source block t is entries t * 32 to (t + 1) * 32 - 1 of q_src_heads, target block j the same entries of q_tgt_heads. With s = 1, source block t shares exactly 8 heads with target block (t + min(1, s - 1)) mod 4 and with each target block (t + k * s) mod 4 for k from 1 to 3, and none with any other. `q_tgt_heads`: see q_src_heads. `kv_tgt_heads`: every key-value head appears exactly twice.
All inputs are finite; a program needn't handle non-finite values.
Results may differ from the reference program's by a relative error of at most 0.001.
Values may be sent and summed in bfloat16 or wider, within the bound.
A program may use at most 256 MiB of HBM per device.

```python
import jax
import jax.numpy as jnp

D = 16384
QH = 128
KVH = 8
HD = 128
TOK = 1024
QDEV = 32
KVT = 4
CDEV = 5120
CAP = 8
NSEL = 4
N_TP = 4


def query_tables(key):
    key = jax.random.fold_in(key, 11)
    key_heads = jax.random.fold_in(key, 0)
    key_group = jax.random.fold_in(key, 2)
    key_order = jax.random.fold_in(key, 3)
    head_order = jax.random.permutation(key_heads, QH).astype(jnp.int32)
    stride = N_TP // NSEL
    steps = jnp.arange(NSEL, dtype=jnp.int32)
    chosen = jnp.where(steps == 0, min(1, stride - 1), steps * stride).astype(jnp.int32)
    grouping = jax.random.permutation(key_group, QDEV).astype(jnp.int32)
    inverse = jnp.argsort(grouping).astype(jnp.int32)
    target_ids = jnp.arange(N_TP, dtype=jnp.int32)[:, None]
    position = jnp.arange(QDEV, dtype=jnp.int32)[None, :]
    source_dev = (target_ids - chosen[position // CAP]) % N_TP
    global_slot = source_dev * QDEV + inverse[position]
    order_keys = jax.random.split(key_order, N_TP)
    shuffle = jax.vmap(lambda k: jax.random.permutation(k, QDEV))(order_keys).astype(jnp.int32)
    global_slot = jnp.take_along_axis(global_slot, shuffle, axis=1)
    target_heads = head_order[global_slot.reshape(QH)]
    return (head_order, target_heads.astype(jnp.int32))


def draw_q_src_heads(key, part):
    return query_tables(key)[0]


def draw_q_tgt_heads(key, part):
    return query_tables(key)[1]


def draw_kv_tgt_heads(key, part):
    order = jax.random.permutation(jax.random.fold_in(key, 23), KVH).astype(jnp.int32)
    fixed_heads = (jnp.arange(KVH, dtype=jnp.int32) + KVH // 2) % KVH
    paired = jnp.stack([fixed_heads, order], axis=1)
    return paired.reshape(2 * KVH).astype(jnp.int32)


def shard_levels(own_key, shape, cuts, smallest, high):
    level, own = 1.0, jax.random.fold_in(own_key, 6)
    for axis_at, parts in cuts:
        heights = jnp.exp(jax.random.uniform(jax.random.fold_in(own, axis_at), (parts,), jnp.float32, smallest / len(cuts), high / len(cuts)))
        level = level * jnp.repeat(heights, shape[axis_at] // parts).reshape([-1 if axis == axis_at else 1 for axis in range(len(shape))])
    return level


def noise(own_key, shape, spread, most, shards=(), kind=jnp.bfloat16):
    factor_of = shard_levels(own_key, shape, shards, -0.22, 0.18) if shards else 1.0
    entries = jax.random.normal(own_key, shape, jnp.float32) * spread * factor_of
    return jnp.minimum(jnp.maximum(entries, -most), most).astype(kind)


def setup_inputs(seed: int = 0, part: int = 0) -> dict:
    key_list = jax.random.split(jax.random.key(seed), 7)
    part_splits = jax.random.split(jax.random.fold_in(key_list[6], part), 7)
    return {
        "acts": noise(part_splits[0], (TOK, D), 1.0, 6.0, ((0, 4), (1, 4))),
        "q_src": noise(part_splits[1], (D, QH * HD), D ** -0.5, 0.046875, ((0, 4), (1, 4))),
        "kv_src": noise(part_splits[2], (D, 2 * KVH * HD), D ** -0.5, 0.046875, ((0, 4), (1, 4))),
        "q_src_heads": draw_q_src_heads(jax.random.fold_in(key_list[6], 71), part),
        "q_tgt_heads": draw_q_tgt_heads(jax.random.fold_in(key_list[6], 71), part),
        "kv_tgt_heads": draw_kv_tgt_heads(jax.random.fold_in(key_list[6], 71), part),
    }


def reference(acts, q_src, kv_src, q_src_heads, q_tgt_heads, kv_tgt_heads):
    head_ids = jnp.arange(QH, dtype=jnp.int32)
    matches = (q_src_heads[None, :] == q_tgt_heads[:, None]).astype(jnp.int32)
    slot_of = jnp.sum(matches * head_ids[None, :], axis=1).astype(jnp.int32)
    q_three = q_src.reshape(D, QH, HD)
    q_new = jnp.take(q_three, slot_of, axis=1).reshape(D, QH * HD)
    kv_three = kv_src.reshape(D, KVH, 2 * HD)
    kv_new = jnp.take(kv_three, kv_tgt_heads, axis=1).reshape(D, 4 * KVH * HD)
    joined_cols = jnp.concatenate([q_new.reshape(D, N_TP, QDEV * HD), kv_new.reshape(D, N_TP, KVT * 2 * HD)], axis=2)
    joined_cols = joined_cols.reshape(D, N_TP * CDEV)
    qkv = jnp.dot(acts, joined_cols, preferred_element_type=jnp.float32).astype(jnp.bfloat16)
    return q_new, kv_new, qkv
```

```python
import functools

import jax
import jax.numpy as jnp
from jax import lax
from jax.experimental import pallas as pl
from jax.experimental.pallas import tpu as pltpu
from jax.sharding import PartitionSpec as P


HD = 128
ROW_CHUNKS = 4
BLOCK_ROWS = 256


def cost(nbytes):
    return pl.CostEstimate(flops=0, bytes_accessed=nbytes, transcendentals=0)


def pack_body(n, cap, pick, x_ref, *outs):
    for o in range(n):
        for r in range(cap):
            start = pl.multiple_of(pick[o * cap + r] * HD, HD)
            outs[o][:, r * HD : (r + 1) * HD] = x_ref[:, pl.ds(start, HD)].astype(outs[o].dtype)


def pack(x, pick, n, cap, first_row, rows):
    width = x.shape[1]
    block = min(BLOCK_ROWS, rows)
    skip = first_row // block
    return pl.pallas_call(
        functools.partial(pack_body, n, cap),
        grid_spec=pltpu.PrefetchScalarGridSpec(
            num_scalar_prefetch=1,
            grid=(rows // block,),
            in_specs=[pl.BlockSpec((block, width), lambda i, p: (skip + i, 0))],
            out_specs=[pl.BlockSpec((block, cap * HD), lambda i, p: (i, 0))] * n,
        ),
        out_shape=[jax.ShapeDtypeStruct((rows, cap * HD), jnp.bfloat16)] * n,
        cost_estimate=cost(rows * (width + n * cap * HD) * 2),
    )(pick, x)


def unpack_body(n, cap, full, has_extra, dest, *refs):
    out = refs[-1]
    for o in range(n):
        for r in range(cap):
            place = dest[o * cap + r]

            def put(o=o, r=r, place=place):
                out[:, pl.ds(pl.multiple_of(place * HD, HD), HD)] = refs[o][:, r * HD : (r + 1) * HD]

            if full:
                put()
            else:
                pl.when(place >= 0)(put)
    if has_extra:
        extra = refs[n]
        out[:, out.shape[1] - extra.shape[1] :] = extra[...].astype(out.dtype)


def unpack(pieces, dest, q_local, cap, first_row, total_rows, before=None, extra=None):
    n, rows = len(pieces), pieces[0].shape[0]
    block = min(BLOCK_ROWS, rows)
    skip = first_row // block
    width = q_local * HD + (extra.shape[1] if extra is not None else 0)
    in_specs = [pl.BlockSpec((block, cap * HD), lambda i, d: (i, 0))] * n
    operands = list(pieces)
    aliases = {}
    if extra is not None:
        in_specs.append(pl.BlockSpec((block, extra.shape[1]), lambda i, d: (i, 0)))
        operands.append(extra)
    if before is not None:
        aliases = {1 + len(operands): 0}
        in_specs.append(pl.BlockSpec(memory_space=pl.ANY))
        operands.append(before)
    return pl.pallas_call(
        functools.partial(unpack_body, n, cap, n * cap == q_local, extra is not None),
        grid_spec=pltpu.PrefetchScalarGridSpec(
            num_scalar_prefetch=1,
            grid=(rows // block,),
            in_specs=in_specs,
            out_specs=pl.BlockSpec((block, width), lambda i, d: (skip + i, 0)),
        ),
        out_shape=jax.ShapeDtypeStruct((total_rows, width), jnp.bfloat16),
        input_output_aliases=aliases,
        cost_estimate=cost(rows * width * 4),
    )(dest, *operands)


def choose_body(n, units, piece_of, unit_of, *refs):
    out = refs[-1]
    for k in range(units):
        for o in range(n):

            @pl.when(piece_of[k] == o)
            def _(k=k, o=o):
                start = pl.multiple_of(unit_of[k] * HD, HD)
                out[:, k * HD : (k + 1) * HD] = refs[o][:, pl.ds(start, HD)]


def choose(pieces, piece_of, unit_of):
    n, (rows, width) = len(pieces), pieces[0].shape
    units = piece_of.shape[0]
    block = min(BLOCK_ROWS, rows)
    return pl.pallas_call(
        functools.partial(choose_body, n, units),
        grid_spec=pltpu.PrefetchScalarGridSpec(
            num_scalar_prefetch=2,
            grid=(rows // block,),
            in_specs=[pl.BlockSpec((block, width), lambda i, a, b: (i, 0))] * n,
            out_specs=pl.BlockSpec((block, units * HD), lambda i, a, b: (i, 0)),
        ),
        out_shape=jax.ShapeDtypeStruct((rows, units * HD), jnp.bfloat16),
        cost_estimate=cost(rows * (n * width + units * HD) * 2),
    )(piece_of, unit_of, *pieces)


def layer(acts, q_src, kv_src, q_src_heads, q_tgt_heads, kv_tgt_heads):
    n = lax.axis_size("tp")
    me = lax.axis_index("tp").astype(jnp.int32)
    rows = q_src.shape[0]
    q_local = q_src.shape[1] // HD
    cap = max(2, q_local // n)

    def swap(x, o):
        return lax.ppermute(x, "tp", [(i, i ^ o) for i in range(n)])

    def exchange(x):
        pieces = {0: x}
        pieces[1] = swap(x, 1)
        for o in range(2, n, 2):
            pieces[o] = swap(x, o)
        for o in range(2, n, 2):
            pieces[o + 1] = swap(pieces[o], 1)
        return [pieces[o] for o in range(n)]

    act_pieces = exchange(acts)
    kv_pieces = exchange(kv_src)

    ids = jnp.arange(q_src_heads.shape[0], dtype=jnp.int32)
    slot_of = jnp.sum(
        jnp.where(q_tgt_heads[:, None] == q_src_heads[None, :], ids[None, :], 0), axis=1
    )
    source_dev = slot_of // q_local
    target_dev = ids // q_local
    earlier = (
        (source_dev[:, None] == source_dev[None, :])
        & (target_dev[:, None] == target_dev[None, :])
        & (ids[None, :] < ids[:, None])
    )
    rank = jnp.sum(earlier.astype(jnp.int32), axis=1)
    buffer_ids = jnp.arange(n * cap, dtype=jnp.int32)
    send_at = jnp.where(source_dev == me, (target_dev ^ me) * cap + rank, -1)
    pick = jnp.sum(
        jnp.where(send_at[None, :] == buffer_ids[:, None], slot_of[None, :] - me * q_local, 0), axis=1
    )
    receive_at = jnp.where(target_dev == me, (source_dev ^ me) * cap + rank, -1)
    dest = (
        jnp.sum(
            jnp.where(
                receive_at[None, :] == buffer_ids[:, None], ids[None, :] - me * q_local + 1, 0
            ),
            axis=1,
        )
        - 1
    )

    chunks = ROW_CHUNKS if rows % (ROW_CHUNKS * BLOCK_ROWS) == 0 else 1
    chunk_rows = rows // chunks
    packed = [pack(q_src, pick, n, cap, c * chunk_rows, chunk_rows) for c in range(chunks)]
    arrived = [[p[0]] + [swap(p[o], o) for o in range(1, n)] for p in packed]

    tokens = acts.shape[0]
    gathered = jnp.zeros((n * tokens, acts.shape[1]), acts.dtype)
    for o in range(n):
        gathered = lax.dynamic_update_slice_in_dim(gathered, act_pieces[o], (me ^ o) * tokens, 0)

    def project(weights):
        full = jnp.dot(gathered, weights, preferred_element_type=jnp.float32)
        return lax.psum_scatter(full, "sub", scatter_dimension=0, tiled=True)

    q_out = project(q_src)

    kv_slots = kv_tgt_heads.shape[0] // n
    per_dev = kv_src.shape[1] // HD
    own_kv = lax.dynamic_slice_in_dim(kv_tgt_heads, me * kv_slots, kv_slots)
    units = (2 * own_kv[:, None] + jnp.arange(2, dtype=jnp.int32)[None, :]).reshape(-1)
    kv_new = choose(kv_pieces, (units // per_dev) ^ me, units % per_dev)
    kv_out = project(kv_new)

    q_new = None
    for c in range(chunks):
        q_new = unpack(arrived[c], dest, q_local, cap, c * chunk_rows, rows, before=q_new)

    out_rows = q_out.shape[0]
    q_packed = pack(q_out, pick, n, cap, 0, out_rows)
    q_moved = [q_packed[0]] + [swap(q_packed[o], o) for o in range(1, n)]
    qkv = unpack(q_moved, dest, q_local, cap, 0, out_rows, extra=kv_out)
    return (q_new, kv_new, qkv)


def solution(mesh):
    in_specs = (
        P(("rep", "tp"), "sub"),
        P(("rep", "sub"), "tp"),
        P(("rep", "sub"), "tp"),
        P(),
        P(),
        P(),
    )
    out_specs = (P(("rep", "sub"), "tp"), P(("rep", "sub"), "tp"), P(("rep", "sub"), "tp"))
    return jax.shard_map(layer, mesh=mesh, in_specs=in_specs, out_specs=out_specs, check_vma=False)
```
